32 devices in a mesh: dp: 2 (over y), tensor: 4 (over x, core), ctx: 4 (over z).
Axes of the slice: x: 2, y: 2, z: 4, core: 2. Of those that a mesh axis runs over, the one named last changes fastest.
Arguments:
- grad_down: bfloat16 [2, 18432, 4608], P('dp', 'tensor', 'ctx'), may hold values from -700 to 700
- grad_query: bfloat16 [2, 4608, 2048], P('dp', 'ctx', 'tensor'), may hold values from -700 to 700
- down_param: float32 [18432, 4608], P(('tensor', 'dp'), 'ctx'), may hold values from -0.3 to 0.3
- down_moment: float32 [18432, 4608], P(('tensor', 'dp'), 'ctx'), may hold values from -6 to 6
- down_second: float32 [4608], P('ctx'), may hold values from 0.1 to 2
- query_param: float32 [4608, 2048], P(('ctx', 'dp'), 'tensor'), may hold values from -0.3 to 0.3
- query_moment: float32 [4608, 2048], P(('ctx', 'dp'), 'tensor'), may hold values from -6 to 6
- query_second: float32 [16], P('tensor'), may hold values from 0.1 to 2
- step_count: int32 [1], replicated, may hold values from 1 to 29
Outputs:
- down_param_new: float32 [18432, 4608], P(('tensor', 'dp'), 'ctx')
- down_moment_new: float32 [18432, 4608], P(('tensor', 'dp'), 'ctx')
- down_second_new: float32 [4608], P('ctx')
- down_update: bfloat16 [18432, 4608], P(('tensor', 'dp'), 'ctx')
- query_param_new: float32 [4608, 2048], P(('ctx', 'dp'), 'tensor')
- query_moment_new: float32 [4608, 2048], P(('ctx', 'dp'), 'tensor')
- query_second_new: float32 [16], P('tensor')
- query_update: bfloat16 [4608, 2048], P(('ctx', 'dp'), 'tensor')
The draws below stay inside these ranges and needn't reach their ends.
All inputs are finite; a program needn't handle non-finite values.
Results may differ from the reference program's by a relative error of at most 0.012.
Values may be sent and summed in bfloat16 or wider, within the bound.
A program may use at most 128 MiB of HBM per device.

```python
import math
import jax
import jax.numpy as jnp
from jax import lax

D = 4608
HEAD_DIM = 128
FF = 18432
HEADS = 16
N_DP = 2


def gradient_field(key, row_count, col_count):
    subkeys = jax.random.split(key, 4)
    row_ramp = jnp.sqrt(3.0) ** (jnp.arange(row_count, dtype=jnp.float32) / row_count)
    row_scale = jnp.exp(jax.random.uniform(subkeys[0], (row_count,), jnp.float32, 0.0, math.log(10.0))) * row_ramp
    col_spread = math.log(10.0)
    col_scale = jnp.exp(jax.random.uniform(subkeys[1], (col_count,), jnp.float32, 0.0, col_spread))
    replica_ramp = jnp.sqrt(3.0) ** (jnp.arange(N_DP, dtype=jnp.float32) / max(N_DP - 1, 1))
    entries = 0.1 * math.sqrt(N_DP) * jax.random.truncated_normal(subkeys[3], -4.0, 4.0, (N_DP, row_count, col_count), jnp.float32)
    return entries * replica_ramp[:, None, None] * row_scale[None, :, None] * col_scale[None, None, :]


def draw_grad_down(key, part):
    return gradient_field(jax.random.fold_in(key, 11), FF, D).astype(jnp.bfloat16)


def draw_grad_query(key, part):
    return gradient_field(jax.random.fold_in(key, 23), D, HEADS * HEAD_DIM).astype(jnp.bfloat16)


def block_levels(key, extent, shards, least, largest):
    def one(axis_at, blocks):
        heights = jax.random.uniform(jax.random.fold_in(jax.random.fold_in(key, 6), axis_at), (blocks,), jnp.float32, least / len(shards), largest / len(shards))
        return jnp.repeat(jnp.exp(heights), extent[axis_at] // blocks).reshape((-1,) + (1,) * (len(extent) - axis_at - 1))

    loudness = one(*shards[0])
    for cut in shards[1:]:
        loudness = loudness * one(*cut)
    return loudness


def gaussian(rng, extent, width, limit, pieces=(), kind=jnp.bfloat16):
    gain = block_levels(rng, extent, pieces, -0.22, 0.18) if pieces else 1.0
    result = jax.random.normal(rng, extent, jnp.float32) * width * gain
    return jnp.minimum(jnp.maximum(result, -limit), limit).astype(kind)


def setup_inputs(seed: int = 0) -> dict:
    keys = jax.random.split(jax.random.key(seed), 10)
    grad_down = draw_grad_down(jax.random.fold_in(keys[9], 71), 0)
    grad_query = draw_grad_query(jax.random.fold_in(keys[9], 71), 0)
    down_param = gaussian(keys[2], (FF, D), 0.05, 0.3, ((0, 8), (1, 4)), jnp.float32)
    down_moment = gaussian(keys[3], (FF, D), 1.0, 6.0, ((0, 8), (1, 4)), jnp.float32)
    down_second = jnp.clip(jnp.exp(math.log(2.0) - 2.9957323 * jax.random.uniform(keys[4], (D,), jnp.float32) ** block_levels(keys[4], (D,), ((0, 4),), -0.2, 0.2)), 0.1, 2.0)
    query_param = gaussian(keys[5], (D, HEADS * HEAD_DIM), 0.05, 0.3, ((0, 8), (1, 4)), jnp.float32)
    query_moment = gaussian(keys[6], (D, HEADS * HEAD_DIM), 1.0, 6.0, ((0, 8), (1, 4)), jnp.float32)
    query_second = jnp.clip(jnp.exp(math.log(2.0) - 2.9957323 * jax.random.uniform(keys[7], (HEADS,), jnp.float32) ** block_levels(keys[7], (HEADS,), ((0, 4),), -0.2, 0.2)), 0.1, 2.0)
    step_count = jax.random.randint(keys[8], (1,), 1, 30).astype(jnp.int32)
    return dict(grad_down=grad_down, grad_query=grad_query, down_param=down_param, down_moment=down_moment, down_second=down_second, query_param=query_param, query_moment=query_moment, query_second=query_second, step_count=step_count)


BETA_ONE = 0.9
BETA_TWO = 0.95
EPSILON = 1e-08
LEARN_RATE = 0.003
DECAY_RATE = 0.1

def replica_mean(gradients):

    def accumulate(position, running_total):
        return running_total + lax.dynamic_index_in_dim(gradients, position, 0, keepdims=False).astype(jnp.float32)
    summed = lax.fori_loop(0, gradients.shape[0], accumulate, jnp.zeros(gradients.shape[1:], jnp.float32))
    return summed / gradients.shape[0]

def finish(parameter, moment, gradient, second_wide, keep_one, keep_two):
    moment_new = BETA_ONE * moment + (1.0 - BETA_ONE) * gradient
    update = moment_new / keep_one / (jnp.sqrt(second_wide / keep_two) + EPSILON)
    parameter_new = parameter - LEARN_RATE * (update + DECAY_RATE * parameter)
    return (parameter_new, moment_new, update.astype(jnp.bfloat16))

def reference(grad_down, grad_query, down_param, down_moment, down_second, query_param, query_moment, query_second, step_count):
    step_value = step_count[0].astype(jnp.float32)
    keep_one = 1.0 - jnp.power(jnp.float32(BETA_ONE), step_value)
    keep_two = 1.0 - jnp.power(jnp.float32(BETA_TWO), step_value)
    down_grad = replica_mean(grad_down)
    query_grad = replica_mean(grad_query)
    neuron_mean = lax.optimization_barrier(jnp.sum(down_grad * down_grad, axis=0)) / FF
    head_mean = lax.optimization_barrier(jnp.sum((query_grad * query_grad).reshape(D, HEADS, HEAD_DIM), axis=(0, 2))) / (D * HEAD_DIM)
    down_second_new = BETA_TWO * down_second + (1.0 - BETA_TWO) * neuron_mean
    query_second_new = BETA_TWO * query_second + (1.0 - BETA_TWO) * head_mean
    down_param_new, down_moment_new, down_update = finish(down_param, down_moment, down_grad, down_second_new[None, :], keep_one, keep_two)
    query_wide = jnp.repeat(query_second_new, HEAD_DIM)
    query_param_new, query_moment_new, query_update = finish(query_param, query_moment, query_grad, query_wide[None, :], keep_one, keep_two)
    return (down_param_new, down_moment_new, down_second_new, down_update, query_param_new, query_moment_new, query_second_new, query_update)
```

```python
import functools

import jax
import jax.numpy as jnp
from jax import lax
from jax.experimental import pallas as pl
from jax.experimental.pallas import tpu as pltpu
from jax.sharding import PartitionSpec as P

HEAD_DIM = 128
LANES = 128

BETA_ONE = 0.9
BETA_TWO = 0.95
EPSILON = 1e-08
LEARN_RATE = 0.003
DECAY_RATE = 0.1

ANY = pl.BlockSpec(memory_space=pl.ANY)


def tile_of(rows, most):
    tile = min(rows, most) // 16 * 16
    while tile > 16 and rows % tile:
        tile -= 16
    return tile if tile and rows % tile == 0 else rows


def pad(width):
    return -(-width // LANES) * LANES


def cost(byte_count, flops=0):
    return pl.CostEstimate(flops=flops, bytes_accessed=byte_count, transcendentals=0)


def cut(gradient, part, first, blocks, rows, after):
    tile = tile_of(rows, 768)
    steps = rows // tile

    def kernel(part_ref, grad_ref, *rest):
        rest[-1][...] = grad_ref[0]

    return pl.pallas_call(
        kernel,
        grid_spec=pltpu.PrefetchScalarGridSpec(
            num_scalar_prefetch=1,
            grid=(blocks, steps),
            in_specs=[pl.BlockSpec((1, tile, LANES), lambda c, i, p: (0, p[0] * steps + i, first + c))]
            + [ANY] * len(after),
            out_specs=pl.BlockSpec((tile, LANES), lambda c, i, p: (i, c)),
        ),
        out_shape=jax.ShapeDtypeStruct((rows, blocks * LANES), gradient.dtype),
        cost_estimate=cost(4 * rows * blocks * LANES),
        name="cut",
    )(part[None], gradient, *after)


def gather_moment(gradient, received, moment, moment_new, me, first, blocks, replicas):
    rows = moment.shape[0]
    tile = tile_of(rows, 768)
    steps = rows // tile
    count = len(received)

    def kernel(me_ref, grad_ref, *rest):
        received_refs, moment_ref = rest[:count], rest[count]
        moment_out, sum_out = rest[-2:]
        total = grad_ref[0].astype(jnp.float32)
        for ref in received_refs:
            total = total + ref[...].astype(jnp.float32)
        mean = total * (1.0 / replicas) if replicas & (replicas - 1) == 0 else total / replicas
        moment_out[...] = BETA_ONE * moment_ref[...] + (1.0 - BETA_ONE) * mean
        squares = jnp.sum(mean * mean, axis=0, keepdims=True)

        @pl.when(pl.program_id(1) == 0)
        def _():
            sum_out[...] = squares

        @pl.when(pl.program_id(1) != 0)
        def _():
            sum_out[...] += squares

    chained = [] if moment_new is None else [moment_new]
    return pl.pallas_call(
        kernel,
        grid_spec=pltpu.PrefetchScalarGridSpec(
            num_scalar_prefetch=1,
            grid=(blocks, steps),
            in_specs=[pl.BlockSpec((1, tile, LANES), lambda c, i, p: (0, p[0] * steps + i, first + c))]
            + [pl.BlockSpec((tile, LANES), lambda c, i, p: (i, c))] * count
            + [pl.BlockSpec((tile, LANES), lambda c, i, p: (i, first + c))]
            + [ANY] * len(chained),
            out_specs=[
                pl.BlockSpec((tile, LANES), lambda c, i, p: (i, first + c)),
                pl.BlockSpec((1, LANES), lambda c, i, p: (0, c)),
            ],
        ),
        out_shape=[
            jax.ShapeDtypeStruct(moment.shape, jnp.float32),
            jax.ShapeDtypeStruct((1, blocks * LANES), jnp.float32),
        ],
        input_output_aliases={3 + count: 0} if chained else {},
        cost_estimate=cost((10 + 2 * count) * rows * blocks * LANES),
        name="gather_moment",
    )(me[None], gradient, *received, moment, *chained)


def finish(keep, second_wide, parameter, moment_new, chained, first, blocks):
    rows = parameter.shape[0]
    tile = tile_of(rows, 768)

    def kernel(keep_ref, second_ref, parameter_ref, moment_ref, *rest):
        parameter_out, update_out = rest[-2:]
        below = jnp.sqrt(second_ref[...] / keep_ref[1]) + EPSILON
        scale = 1.0 / (keep_ref[0] * below)
        update = moment_ref[...] * scale
        value = parameter_ref[...]
        parameter_out[...] = value - LEARN_RATE * (update + DECAY_RATE * value)
        update_out[...] = update.astype(jnp.bfloat16)

    wide = pl.BlockSpec((tile, LANES), lambda c, i: (i, first + c))
    aliases = {3: 0}
    if chained:
        aliases.update({4: 1, 5: 2})
    return pl.pallas_call(
        kernel,
        grid=(blocks, rows // tile),
        in_specs=[
            pl.BlockSpec(memory_space=pltpu.SMEM),
            pl.BlockSpec((1, LANES), lambda c, i: (0, c)),
            wide,
            wide,
        ]
        + [ANY] * len(chained),
        out_specs=[ANY, wide, wide],
        out_shape=[
            jax.ShapeDtypeStruct(parameter.shape, jnp.float32),
            jax.ShapeDtypeStruct(parameter.shape, jnp.float32),
            jax.ShapeDtypeStruct(parameter.shape, jnp.bfloat16),
        ],
        input_output_aliases=aliases,
        cost_estimate=cost(14 * rows * blocks * LANES),
        name="finish",
    )(keep, second_wide, parameter, moment_new, *chained)


def total_over(value, axes):
    size = 1
    for axis in axes:
        size *= lax.axis_size(axis)
    if size > 8 or size & (size - 1):
        return lax.psum(value, axes)
    terms = [value] + [
        lax.ppermute(value, axes, [(i, i ^ k) for i in range(size)]) for k in range(1, size)
    ]
    while len(terms) > 1:
        terms = [a + b for a, b in zip(terms[::2], terms[1::2])]
    return terms[0]


def exchange(gradient, rows, first, blocks, me, after):
    replicas = lax.axis_size("dp")
    received = []
    for d in range(1, replicas):
        part = lax.rem(me + d, replicas)
        piece = cut(gradient, part, first, blocks, rows, after)
        received.append(lax.ppermute(piece, "dp", [(i, (i + d) % replicas) for i in range(replicas)]))
    return received


def plan(blocks):
    sizes, left = [], blocks
    while left > 3:
        sizes.append(min(2, left - 3))
        left -= sizes[-1]
    early = len(sizes)
    return sizes + [1] * left, early


def shards(
    grad_down,
    grad_query,
    down_param,
    down_moment,
    down_second,
    query_param,
    query_moment,
    query_second,
    step_count,
):
    replicas = lax.axis_size("dp")
    me = lax.axis_index("dp").astype(jnp.int32)
    step_value = step_count[0].astype(jnp.float32)
    keep = jnp.stack(
        [
            1.0 - jnp.power(jnp.float32(BETA_ONE), step_value),
            1.0 - jnp.power(jnp.float32(BETA_TWO), step_value),
        ]
    )
    down_rows, down_cols = down_param.shape
    query_rows, query_cols = query_param.shape
    neuron_count = grad_down.shape[1] * lax.axis_size("tensor")
    head_count = grad_query.shape[1] * lax.axis_size("ctx") * HEAD_DIM
    query_blocks = query_cols // LANES

    sizes, early = plan(pad(down_cols) // LANES)
    starts = [sum(sizes[:k]) for k in range(len(sizes))]

    query_received = exchange(grad_query, query_rows, 0, query_blocks, me, [])
    down_received = [exchange(grad_down, down_rows, starts[k], sizes[k], me, []) for k in range(min(2, len(sizes)))]

    query_moment_new, query_sum = gather_moment(
        grad_query, query_received, query_moment, None, me, 0, query_blocks, replicas
    )
    done = [query_sum]
    down_moment_new = None
    down_sums = []
    groups = [(0, early), (early, len(sizes) - 1), (len(sizes) - 1, len(sizes))]
    groups = [g for g in groups if g[0] < g[1]]
    seconds = []
    chained = []
    pending = None
    for k in range(len(sizes)):
        if k + 2 < len(sizes):
            down_received.append(exchange(grad_down, down_rows, starts[k + 2], sizes[k + 2], me, done))
        down_moment_new, squares = gather_moment(
            grad_down, down_received[k], down_moment, down_moment_new, me, starts[k], sizes[k], replicas
        )
        down_sums.append(squares)
        done = [squares]
        for low, high in groups:
            if high != k + 1:
                continue
            begin = starts[low] * LANES
            end = min(begin + sum(sizes[low:high]) * LANES, down_cols)
            part = jnp.concatenate(down_sums[low:high], axis=1)
            total = total_over(part, ("dp", "tensor"))
            old = jnp.pad(down_second[begin:end], (0, part.shape[1] - (end - begin)))[None]
            second = BETA_TWO * old + (1.0 - BETA_TWO) * (total / neuron_count)
            seconds.append(second[0, : end - begin])
            if pending is not None:
                down_moment_new, *chained = finish(
                    keep, pending[0], down_param, down_moment_new, chained, pending[1], pending[2]
                )
            pending = (second, starts[low], sum(sizes[low:high]))
            if low == 0:
                head_part = jnp.sum(query_sum.reshape(query_blocks, HEAD_DIM), axis=1)[None]
                head_total = total_over(head_part, ("dp", "ctx"))[0]
                query_second_new = BETA_TWO * query_second + (1.0 - BETA_TWO) * (head_total / head_count)
                query_moment_new, query_param_new, query_update = finish(
                    keep,
                    jnp.repeat(query_second_new, HEAD_DIM)[None],
                    query_param,
                    query_moment_new,
                    [],
                    0,
                    query_blocks,
                )
    down_moment_new, *chained = finish(
        keep, pending[0], down_param, down_moment_new, chained, pending[1], pending[2]
    )
    down_param_new, down_update = chained
    return (
        down_param_new,
        down_moment_new,
        jnp.concatenate(seconds),
        down_update,
        query_param_new,
        query_moment_new,
        query_second_new,
        query_update,
    )


def solution(mesh):
    in_specs = (
        P("dp", "tensor", "ctx"),
        P("dp", "ctx", "tensor"),
        P(("tensor", "dp"), "ctx"),
        P(("tensor", "dp"), "ctx"),
        P("ctx"),
        P(("ctx", "dp"), "tensor"),
        P(("ctx", "dp"), "tensor"),
        P("tensor"),
        P(),
    )
    out_specs = (
        P(("tensor", "dp"), "ctx"),
        P(("tensor", "dp"), "ctx"),
        P("ctx"),
        P(("tensor", "dp"), "ctx"),
        P(("ctx", "dp"), "tensor"),
        P(("ctx", "dp"), "tensor"),
        P("tensor"),
        P(("ctx", "dp"), "tensor"),
    )
    return jax.shard_map(shards, mesh=mesh, in_specs=in_specs, out_specs=out_specs, check_vma=False)
```

```python
import functools

import jax
import jax.numpy as jnp
from jax import lax
from jax.experimental import pallas as pl
from jax.experimental.pallas import tpu as pltpu
from jax.sharding import PartitionSpec as P


HEAD_DIM = 128
LANES = 128

BETA_ONE = 0.9
BETA_TWO = 0.95
EPSILON = 1e-08
LEARN_RATE = 0.003
DECAY_RATE = 0.1


ANY = pl.BlockSpec(memory_space=pl.ANY)


def tile_of(rows, most):
    tile = min(rows, most) // 16 * 16
    while tile > 16 and rows % tile:
        tile -= 16
    return tile if tile and rows % tile == 0 else rows


def pad(width):
    return -(-width // LANES) * LANES


def cost(byte_count, flops=0):
    return pl.CostEstimate(flops=flops, bytes_accessed=byte_count, transcendentals=0)


def cut(gradient, part, first, blocks, rows, after):
    tile = tile_of(rows, 768)
    steps = rows // tile

    def kernel(part_ref, grad_ref, *rest):
        rest[-1][...] = grad_ref[0]

    return pl.pallas_call(
        kernel,
        grid_spec=pltpu.PrefetchScalarGridSpec(
            num_scalar_prefetch=1,
            grid=(blocks, steps),
            in_specs=[pl.BlockSpec((1, tile, LANES), lambda c, i, p: (0, p[0] * steps + i, first + c))]
            + [ANY] * len(after),
            out_specs=pl.BlockSpec((tile, LANES), lambda c, i, p: (i, c)),
        ),
        out_shape=jax.ShapeDtypeStruct((rows, blocks * LANES), gradient.dtype),
        cost_estimate=cost(4 * rows * blocks * LANES),
        name="cut",
    )(part[None], gradient, *after)


def gather_moment(gradient, received, moment, moment_new, me, first, blocks, replicas):
    rows = moment.shape[0]
    tile = tile_of(rows, 768)
    steps = rows // tile
    count = len(received)

    def kernel(me_ref, grad_ref, *rest):
        received_refs, moment_ref = rest[:count], rest[count]
        moment_out, sum_out = rest[-2:]
        total = grad_ref[0].astype(jnp.float32)
        top = pl.multiple_of(pl.program_id(1) * tile, tile)
        side = pl.multiple_of(pl.program_id(0) * LANES, LANES)
        for ref in received_refs:
            total = total + ref[pl.ds(top, tile), pl.ds(side, LANES)].astype(jnp.float32)
        mean = total * (1.0 / replicas) if replicas & (replicas - 1) == 0 else total / replicas
        moment_out[...] = BETA_ONE * moment_ref[...] + (1.0 - BETA_ONE) * mean
        squares = jnp.sum(mean * mean, axis=0, keepdims=True)

        @pl.when(pl.program_id(1) == 0)
        def _():
            sum_out[...] = squares

        @pl.when(pl.program_id(1) != 0)
        def _():
            sum_out[...] += squares

    chained = [] if moment_new is None else [moment_new]
    return pl.pallas_call(
        kernel,
        grid_spec=pltpu.PrefetchScalarGridSpec(
            num_scalar_prefetch=1,
            grid=(blocks, steps),
            in_specs=[pl.BlockSpec((1, tile, LANES), lambda c, i, p: (0, p[0] * steps + i, first + c))]
            + [pl.BlockSpec(memory_space=pltpu.VMEM)] * count
            + [pl.BlockSpec((tile, LANES), lambda c, i, p: (i, first + c))]
            + [ANY] * len(chained),
            out_specs=[
                pl.BlockSpec((tile, LANES), lambda c, i, p: (i, first + c)),
                pl.BlockSpec((1, LANES), lambda c, i, p: (0, c)),
            ],
        ),
        out_shape=[
            jax.ShapeDtypeStruct(moment.shape, jnp.float32),
            jax.ShapeDtypeStruct((1, blocks * LANES), jnp.float32),
        ],
        input_output_aliases={3 + count: 0} if chained else {},
        cost_estimate=cost((10 + 2 * count) * rows * blocks * LANES),
        name="gather_moment",
    )(me[None], gradient, *received, moment, *chained)


def finish(keep, second_wide, parameter, moment_new, chained, first, blocks):
    rows = parameter.shape[0]
    tile = tile_of(rows, 768)

    def kernel(keep_ref, second_ref, parameter_ref, moment_ref, *rest):
        parameter_out, update_out = rest[-2:]
        below = jnp.sqrt(second_ref[...] / keep_ref[1]) + EPSILON
        scale = 1.0 / (keep_ref[0] * below)
        update = moment_ref[...] * scale
        value = parameter_ref[...]
        parameter_out[...] = value - LEARN_RATE * (update + DECAY_RATE * value)
        update_out[...] = update.astype(jnp.bfloat16)

    wide = pl.BlockSpec((tile, LANES), lambda c, i: (i, first + c))
    aliases = {3: 0}
    if chained:
        aliases.update({4: 1, 5: 2})
    return pl.pallas_call(
        kernel,
        grid=(blocks, rows // tile),
        in_specs=[
            pl.BlockSpec(memory_space=pltpu.SMEM),
            pl.BlockSpec((1, LANES), lambda c, i: (0, c)),
            wide,
            wide,
        ]
        + [ANY] * len(chained),
        out_specs=[ANY, wide, wide],
        out_shape=[
            jax.ShapeDtypeStruct(parameter.shape, jnp.float32),
            jax.ShapeDtypeStruct(parameter.shape, jnp.float32),
            jax.ShapeDtypeStruct(parameter.shape, jnp.bfloat16),
        ],
        input_output_aliases=aliases,
        cost_estimate=cost(14 * rows * blocks * LANES),
        name="finish",
    )(keep, second_wide, parameter, moment_new, *chained)


def total_over(value, axes):
    size = 1
    for axis in axes:
        size *= lax.axis_size(axis)
    if size > 8 or size & (size - 1):
        return lax.psum(value, axes)
    terms = [value] + [
        lax.ppermute(value, axes, [(i, i ^ k) for i in range(size)]) for k in range(1, size)
    ]
    while len(terms) > 1:
        terms = [a + b for a, b in zip(terms[::2], terms[1::2])]
    return terms[0]


def peer_of(axes, sizes, step):
    coordinates = {}
    for axis, size in reversed(list(zip(axes, sizes))):
        index, bits = lax.axis_index(axis), step % size
        step //= size
        bit = 1
        while bit < size:
            if bits & bit:
                index = index + bit - 2 * bit * (index // bit % 2)
            bit *= 2
        coordinates[axis] = index
    return coordinates


def spread(values, axes_of, collective_id):
    sizes_of = [tuple(lax.axis_size(axis) for axis in axes) for axes in axes_of]
    counts = [functools.reduce(lambda a, b: a * b, sizes) for sizes in sizes_of]
    number = len(values)

    def kernel(*refs):
        value_refs, out_refs = refs[:number], refs[number : 2 * number]
        slot_refs = refs[2 * number : 3 * number]
        send_refs, recv_refs = refs[3 * number : 4 * number], refs[4 * number :]
        barrier = pltpu.get_barrier_semaphore()
        for n in range(number):
            for k in range(1, counts[n]):
                pl.semaphore_signal(
                    barrier,
                    inc=1,
                    device_id=peer_of(axes_of[n], sizes_of[n], k),
                    device_id_type=pl.DeviceIdType.MESH,
                )
        pl.semaphore_wait(barrier, sum(counts) - number)
        copies = []
        for n in range(number):
            for k in range(1, counts[n]):
                copy = pltpu.make_async_remote_copy(
                    src_ref=value_refs[n],
                    dst_ref=slot_refs[n].at[k - 1],
                    send_sem=send_refs[n].at[k - 1],
                    recv_sem=recv_refs[n].at[k - 1],
                    device_id=peer_of(axes_of[n], sizes_of[n], k),
                    device_id_type=pl.DeviceIdType.MESH,
                )
                copy.start()
                copies.append(copy)
        for copy in copies:
            copy.wait()
        for n in range(number):
            terms = [value_refs[n][...]] + [slot_refs[n][k - 1] for k in range(1, counts[n])]
            while len(terms) > 1:
                terms = [a + b for a, b in zip(terms[::2], terms[1::2])]
            out_refs[n][...] = terms[0]

    vmem = pl.BlockSpec(memory_space=pltpu.VMEM)
    semaphores = [pltpu.SemaphoreType.DMA((max(count - 1, 1),)) for count in counts]
    return pl.pallas_call(
        kernel,
        in_specs=[vmem] * number,
        out_specs=[vmem] * number,
        out_shape=[jax.ShapeDtypeStruct(value.shape, value.dtype) for value in values],
        scratch_shapes=[
            pltpu.VMEM((max(count - 1, 1),) + value.shape, value.dtype) for count, value in zip(counts, values)
        ]
        + semaphores
        + semaphores,
        compiler_params=pltpu.CompilerParams(collective_id=collective_id, has_side_effects=True),
        cost_estimate=cost(8000000),
        name="spread",
    )(*values)


def held(piece, after):
    def kernel(*refs):
        pass

    return pl.pallas_call(
        kernel,
        in_specs=[ANY] * (1 + len(after)),
        out_specs=ANY,
        out_shape=jax.ShapeDtypeStruct(piece.shape, piece.dtype),
        input_output_aliases={0: 0},
        cost_estimate=cost(1000),
        name="held",
    )(piece, *after)


def pieces_of(gradient, rows, first, blocks, me):
    replicas = lax.axis_size("dp")
    return [cut(gradient, lax.rem(me + d, replicas), first, blocks, rows, []) for d in range(1, replicas)]


def send(pieces, after):
    replicas = lax.axis_size("dp")
    received = []
    for d, piece in enumerate(pieces, 1):
        piece = held(piece, after) if after else piece
        received.append(lax.ppermute(piece, "dp", [(i, (i + d) % replicas) for i in range(replicas)]))
    return received


def plan(blocks):
    sizes, left = [], blocks
    while left > 3:
        sizes.append(min(2, left - 3))
        left -= sizes[-1]
    early = max(len(sizes) - 1, 1)
    middle = max(len(sizes), early)
    sizes += [1] * left
    groups = [(0, early), (early, middle), (middle, len(sizes))]
    return sizes, [group for group in groups if group[0] < group[1]]


def shards(
    grad_down,
    grad_query,
    down_param,
    down_moment,
    down_second,
    query_param,
    query_moment,
    query_second,
    step_count,
):
    replicas = lax.axis_size("dp")
    me = lax.axis_index("dp").astype(jnp.int32)
    step_value = step_count[0].astype(jnp.float32)
    keep = jnp.stack(
        [
            1.0 - jnp.power(jnp.float32(BETA_ONE), step_value),
            1.0 - jnp.power(jnp.float32(BETA_TWO), step_value),
        ]
    )
    down_rows, down_cols = down_param.shape
    query_rows, query_cols = query_param.shape
    neuron_count = grad_down.shape[1] * lax.axis_size("tensor")
    head_count = grad_query.shape[1] * lax.axis_size("ctx") * HEAD_DIM
    query_blocks = query_cols // LANES

    sizes, groups = plan(pad(down_cols) // LANES)
    starts = [sum(sizes[:k]) for k in range(len(sizes))]

    query_pieces = pieces_of(grad_query, query_rows, 0, query_blocks, me)
    query_received = send(query_pieces, [])
    pieces = [pieces_of(grad_down, down_rows, starts[k], sizes[k], me) for k in range(len(sizes))]
    down_received = [send(pieces[0], [])]

    query_moment_new, query_sum = gather_moment(
        grad_query, query_received, query_moment, None, me, 0, query_blocks, replicas
    )
    if len(sizes) > 1:
        down_received.append(send(pieces[1], [query_sum]))
    down_moment_new = None
    down_sums, seconds, chained, waiting = [], [], [], []
    for k in range(len(sizes)):
        down_moment_new, squares = gather_moment(
            grad_down, down_received[k], down_moment, down_moment_new, me, starts[k], sizes[k], replicas
        )
        down_sums.append(squares)
        done = [squares]
        for number, (low, high) in enumerate(groups):
            if high != k + 1:
                continue
            width = sum(sizes[low:high]) * LANES
            part = jnp.concatenate(down_sums[low:high], axis=1)
            values, axes_of = [part], [("tensor",)]
            if high == len(sizes):
                axes_of = [("dp", "tensor")]
            if low == 0:
                values.append(query_sum)
                axes_of.append(("dp", "ctx") if high == len(sizes) else ("ctx",))
            totals = spread(values, axes_of, number)
            done = [totals[0]]
            joined = jnp.concatenate(totals, axis=1)
            if high < len(sizes):
                joined = total_over(joined, ("dp",))
            waiting.append((joined, low, high, width))
        ahead = k + 4 if k + 4 == len(sizes) else k + 3
        while len(down_received) < min(ahead, len(sizes)):
            down_received.append(send(pieces[len(down_received)], done))
        while waiting and (k + 1 == len(sizes) or waiting[0][2] + (2 if waiting[0][1] else 1) <= k + 1):
            joined, low, high, width = waiting.pop(0)
            begin = starts[low] * LANES
            end = min(begin + width, down_cols)
            old = jnp.pad(down_second[begin:end], (0, width - (end - begin)))[None]
            second = BETA_TWO * old + (1.0 - BETA_TWO) * (joined[:, :width] / neuron_count)
            seconds.append(second[0, : end - begin])
            down_moment_new, *chained = finish(
                keep, second, down_param, down_moment_new, chained, starts[low], sum(sizes[low:high])
            )
            if low == 0:
                head_total = jnp.sum(joined[0, width:].reshape(-1, HEAD_DIM), axis=1)
                query_second_new = BETA_TWO * query_second + (1.0 - BETA_TWO) * (head_total / head_count)
                query_moment_new, query_param_new, query_update = finish(
                    keep,
                    jnp.repeat(query_second_new, HEAD_DIM)[None],
                    query_param,
                    query_moment_new,
                    [],
                    0,
                    query_blocks,
                )
    down_param_new, down_update = chained
    return (
        down_param_new,
        down_moment_new,
        jnp.concatenate(seconds),
        down_update,
        query_param_new,
        query_moment_new,
        query_second_new,
        query_update,
    )


def solution(mesh):
    in_specs = (
        P("dp", "tensor", "ctx"),
        P("dp", "ctx", "tensor"),
        P(("tensor", "dp"), "ctx"),
        P(("tensor", "dp"), "ctx"),
        P("ctx"),
        P(("ctx", "dp"), "tensor"),
        P(("ctx", "dp"), "tensor"),
        P("tensor"),
        P(),
    )
    out_specs = (
        P(("tensor", "dp"), "ctx"),
        P(("tensor", "dp"), "ctx"),
        P("ctx"),
        P(("tensor", "dp"), "ctx"),
        P(("ctx", "dp"), "tensor"),
        P(("ctx", "dp"), "tensor"),
        P("tensor"),
        P(("ctx", "dp"), "tensor"),
    )

    return jax.shard_map(shards, mesh=mesh, in_specs=in_specs, out_specs=out_specs, check_vma=False)
```
